8 devices in a mesh: part: 1 (over z), model: 2 (over y), data: 4 (over x, core).
Axes of the slice: x: 2, y: 2, z: 1, core: 2. Of those that a mesh axis runs over, the one named last changes fastest.
Arguments:
- hidden: bfloat16 [128, 1, 3840], P(('part', 'data'))
- positions: int32 [128], P(('part', 'data'))
- k_local: bfloat16 [128, 64, 8, 256], P(('part', 'data'), None, 'model')
- v_local: bfloat16 [128, 64, 8, 256], P(('part', 'data'), None, 'model')
- k_global: bfloat16 [128, 256, 8, 256], P(('part', 'data'), None, 'model')
- v_global: bfloat16 [128, 256, 8, 256], P(('part', 'data'), None, 'model')
- w_q: bfloat16 [2, 3840, 16, 256], P(None, 'data', 'model')
- w_k: bfloat16 [2, 3840, 8, 256], P(None, 'data', 'model')
- w_v: bfloat16 [2, 3840, 8, 256], P(None, 'data', 'model')
- w_o: bfloat16 [2, 16, 256, 3840], P(None, 'model', None, 'data')
- w_gate: bfloat16 [2, 3840, 15360], P(None, 'data', 'model')
- w_up: bfloat16 [2, 3840, 15360], P(None, 'data', 'model')
- w_down: bfloat16 [2, 15360, 3840], P(None, 'model', 'data')
- norm_gains: bfloat16 [2, 4, 3840], replicated
Outputs:
- output 1: bfloat16 [128, 1, 3840], P(('part', 'data'))
- output 2: bfloat16 [128, 64, 8, 256], P(('part', 'data'), None, 'model')
- output 3: bfloat16 [128, 64, 8, 256], P(('part', 'data'), None, 'model')
- output 4: bfloat16 [128, 256, 8, 256], P(('part', 'data'), None, 'model')
- output 5: bfloat16 [128, 256, 8, 256], P(('part', 'data'), None, 'model')
All inputs are finite; a program needn't handle non-finite values.
Results may differ from the reference program's by a relative error of at most 0.02.
Values are sent between devices in bfloat16 or wider.
A program may use at most 1 GiB of HBM per device.

```python
import jax
import jax.numpy as jnp
from jax import lax

MODEL_DIM = 3840
NUM_HEADS = 16
NUM_KV = 8
HEAD_DIM = 256
FF_DIM = 15360
WINDOW = 64
CTX_LEN = 256
BATCH = 128

HEAD_GROUP = NUM_HEADS // NUM_KV
SOFT_CAP = 50.0
NORM_EPS = 1e-6
ROPE_BASE = 10000.0
QK_SCALE = 6.0


def setup_inputs(seed: int = 0, part: int = 0) -> dict:
    base_key = jax.random.key(seed)
    weight_keys = jax.random.split(base_key, 8)
    part_keys = jax.random.split(jax.random.fold_in(base_key, part), 6)

    def normal_bf16(rng_key, arr_shape, factor):
        return (factor * jax.random.normal(rng_key, arr_shape, jnp.float32)).astype(jnp.bfloat16)

    raw_pos = jax.random.randint(part_keys[0], (BATCH,), 0, CTX_LEN)
    row_ids = jnp.arange(BATCH)
    positions = jnp.where(row_ids == 0, CTX_LEN - 1, jnp.where(row_ids == BATCH // 2, raw_pos % WINDOW, raw_pos)).astype(jnp.int32)
    kv_local = (BATCH, WINDOW, NUM_KV, HEAD_DIM)
    kv_global = (BATCH, CTX_LEN, NUM_KV, HEAD_DIM)
    in_scale = MODEL_DIM ** -0.5
    return {
        "hidden": normal_bf16(part_keys[1], (BATCH, 1, MODEL_DIM), 1.0),
        "positions": positions,
        "k_local": normal_bf16(part_keys[2], kv_local, QK_SCALE),
        "v_local": normal_bf16(part_keys[3], kv_local, 1.0),
        "k_global": normal_bf16(part_keys[4], kv_global, QK_SCALE),
        "v_global": normal_bf16(part_keys[5], kv_global, 1.0),
        "w_q": normal_bf16(weight_keys[0], (2, MODEL_DIM, NUM_HEADS, HEAD_DIM), QK_SCALE * in_scale),
        "w_k": normal_bf16(weight_keys[1], (2, MODEL_DIM, NUM_KV, HEAD_DIM), QK_SCALE * in_scale),
        "w_v": normal_bf16(weight_keys[2], (2, MODEL_DIM, NUM_KV, HEAD_DIM), in_scale),
        "w_o": normal_bf16(weight_keys[3], (2, NUM_HEADS, HEAD_DIM, MODEL_DIM), (NUM_HEADS * HEAD_DIM) ** -0.5),
        "w_gate": normal_bf16(weight_keys[4], (2, MODEL_DIM, FF_DIM), in_scale),
        "w_up": normal_bf16(weight_keys[5], (2, MODEL_DIM, FF_DIM), in_scale),
        "w_down": normal_bf16(weight_keys[6], (2, FF_DIM, MODEL_DIM), FF_DIM ** -0.5),
        "norm_gains": normal_bf16(weight_keys[7], (2, 4, MODEL_DIM), 0.5),
    }


def rms_norm(hidden, gain):
    mean_sq = jnp.mean(jnp.square(hidden), axis=-1, keepdims=True)
    return hidden * lax.rsqrt(mean_sq + NORM_EPS) * (1.0 + gain.astype(jnp.float32))


def rotary(hidden, cos_t, sin_t):
    half_dim = hidden.shape[-1] // 2
    first_half = hidden[..., :half_dim]
    second_half = hidden[..., half_dim:]
    return jnp.concatenate([first_half * cos_t - second_half * sin_t, second_half * cos_t + first_half * sin_t], axis=-1)


def rope_tables(positions):
    inv_freq = ROPE_BASE ** (-jnp.arange(0, HEAD_DIM, 2).astype(jnp.float32) / HEAD_DIM)
    angles = positions.astype(jnp.float32)[:, None] * inv_freq[None, :]
    return jnp.cos(angles)[:, None, :], jnp.sin(angles)[:, None, :]


def attend_row(operands):
    q_row, k_row, v_row, valid_row = operands
    q_grp = q_row.reshape(NUM_KV, HEAD_GROUP, HEAD_DIM).astype(jnp.float32)
    scores = jnp.einsum("kgd,tkd->kgt", q_grp, k_row.astype(jnp.float32))
    scores = SOFT_CAP * jnp.tanh(scores / SOFT_CAP)
    scores = jnp.where(valid_row[None, None, :], scores, -1e30)
    attn_prob = jax.nn.softmax(scores, axis=-1).astype(jnp.bfloat16)
    head_out = jnp.einsum("kgt,tkd->kgd", attn_prob.astype(jnp.float32), v_row.astype(jnp.float32))
    return head_out.astype(jnp.bfloat16).reshape(NUM_HEADS, HEAD_DIM)


def decoder_layer(hidden, positions, k_cache, v_cache, weights, layer, is_local):
    w_q, w_k, w_v, w_o, w_gate, w_up, w_down, norm_gains = weights
    layer_gains = norm_gains[layer]
    residual = hidden[:, 0, :].astype(jnp.float32)
    normed = rms_norm(residual, layer_gains[0]).astype(jnp.bfloat16)
    q_proj = jnp.dot(normed, w_q[layer].reshape(MODEL_DIM, NUM_HEADS * HEAD_DIM), preferred_element_type=jnp.float32).reshape(BATCH, NUM_HEADS, HEAD_DIM)
    k_proj = jnp.dot(normed, w_k[layer].reshape(MODEL_DIM, NUM_KV * HEAD_DIM), preferred_element_type=jnp.float32).reshape(BATCH, NUM_KV, HEAD_DIM)
    v_proj = jnp.dot(normed, w_v[layer].reshape(MODEL_DIM, NUM_KV * HEAD_DIM), preferred_element_type=jnp.float32).reshape(BATCH, NUM_KV, HEAD_DIM)
    cos_t, sin_t = rope_tables(positions)
    q_new = (rotary(q_proj, cos_t, sin_t) * HEAD_DIM ** -0.5).astype(jnp.bfloat16)
    k_new = rotary(k_proj, cos_t, sin_t).astype(jnp.bfloat16)
    v_new = v_proj.astype(jnp.bfloat16)
    cache_len = k_cache.shape[1]
    slot_ids = jnp.arange(cache_len)
    if is_local:
        slot_now = positions % cache_len
        valid_mask = ((positions[:, None] - slot_ids[None, :]) % cache_len) <= positions[:, None]
    else:
        slot_now = positions
        valid_mask = slot_ids[None, :] <= positions[:, None]
    slot_hit = (slot_ids[None, :] == slot_now[:, None])[:, :, None, None]
    k_cache = jnp.where(slot_hit, k_new[:, None], k_cache)
    v_cache = jnp.where(slot_hit, v_new[:, None], v_cache)
    head_out = lax.map(attend_row, (q_new, k_cache, v_cache, valid_mask))
    attn_sum = jnp.dot(head_out.reshape(BATCH, NUM_HEADS * HEAD_DIM), w_o[layer].reshape(NUM_HEADS * HEAD_DIM, MODEL_DIM), preferred_element_type=jnp.float32)
    mid_hidden = (residual + rms_norm(attn_sum, layer_gains[1])).astype(jnp.bfloat16)
    mid_f = mid_hidden.astype(jnp.float32)
    normed_ff = rms_norm(mid_f, layer_gains[2]).astype(jnp.bfloat16)
    gate_proj = jnp.dot(normed_ff, w_gate[layer], preferred_element_type=jnp.float32)
    up_proj = jnp.dot(normed_ff, w_up[layer], preferred_element_type=jnp.float32)
    gated_act = (jax.nn.gelu(gate_proj, approximate=True) * up_proj).astype(jnp.bfloat16)
    down_sum = jnp.dot(gated_act, w_down[layer], preferred_element_type=jnp.float32)
    layer_out = (mid_f + rms_norm(down_sum, layer_gains[3])).astype(jnp.bfloat16)
    return layer_out[:, None, :], k_cache, v_cache


def reference(hidden, positions, k_local, v_local, k_global, v_global, w_q, w_k, w_v, w_o, w_gate, w_up, w_down, norm_gains):
    weights = (w_q, w_k, w_v, w_o, w_gate, w_up, w_down, norm_gains)
    mid_hidden, k_local, v_local = decoder_layer(hidden, positions, k_local, v_local, weights, 0, True)
    final, k_global, v_global = decoder_layer(mid_hidden, positions, k_global, v_global, weights, 1, False)
    return (final, k_local, v_local, k_global, v_global)
```

```python
import functools

import jax
import jax.numpy as jnp
from jax import lax
from jax.experimental import pallas as pl
from jax.experimental.pallas import tpu as pltpu
from jax.sharding import PartitionSpec as P

SOFT_CAP = 50.0
NORM_EPS = 1e-6
ROPE_BASE = 10000.0

ROW_SPEC = P(("part", "data"), None, None)
POS_SPEC = P(("part", "data"))
CACHE_SPEC = P(("part", "data"), None, "model", None)
PROJ_IN_SPEC = P(None, "data", "model", None)
PROJ_OUT_SPEC = P(None, "model", None, "data")
FF_IN_SPEC = P(None, "data", "model")
FF_OUT_SPEC = P(None, "model", "data")
GAIN_SPEC = P(None, None, None)

MESH = pl.DeviceIdType.MESH
F32, BF16 = jnp.float32, jnp.bfloat16

ROWS = 32
OWN = 16
ALL = 128
WID = 960
FF = 7680
CH = 768
NC = FF // CH
WSLOTS = 3
QW = 4096
QCH = 1024
NQ = QW // QCH
OCH = 1024
NO = 2
NT = (((1,), (1,)), ((), ()))


class Place:
    def __init__(self):
        self.m = lax.axis_index("model")
        self.d = lax.axis_index("data")
        self.x = self.d // 2
        self.c = self.d % 2
        self.me = self.m * 4 + self.d
        self.block = self.c * 2 + self.x
        self.xblock = self.c * 2 + (1 - self.x)
        self.xpeer = {"model": self.m, "data": (1 - self.x) * 2 + self.c}
        self.partner = {"model": self.m, "data": self.x * 2 + (1 - self.c)}

    def other(self, o):
        om, ox, oc = o // 4, (o // 2) % 2, o % 2
        flip = lambda v, b: (1 - v) if b else v
        m, x, c = flip(self.m, om), flip(self.x, ox), flip(self.c, oc)
        return m, x, c, {"model": m, "data": x * 2 + c}


def rcopy(src, dst, ssem, rsem, dev):
    return pltpu.make_async_remote_copy(src_ref=src, dst_ref=dst, send_sem=ssem, recv_sem=rsem, device_id=dev, device_id_type=MESH)


def rows_at(start, size):
    return pl.ds(pl.multiple_of(start, size), size)


def barrier_all(pc):
    sem = pltpu.get_barrier_semaphore()
    for o in range(1, 8):
        pl.semaphore_signal(sem, inc=1, device_id=pc.other(o)[3], device_id_type=MESH)
    pl.semaphore_wait(sem, 7)


def spread_rows(pc, parts, hsend, hall, ssem, rsem):
    for i in range(4):
        hsend[i] = parts[i]
    mine = rows_at(pc.block * ROWS + pc.m * OWN, OWN)
    copies = []
    for o in range(1, 8):
        m, x, c, dev = pc.other(o)
        cp = rcopy(hsend.at[x * 2 + c], hall.at[mine, :], ssem.at[o], rsem.at[o], dev)
        cp.start()
        copies.append(cp)
    hall[mine, :] = hsend[pc.d]
    for cp in copies:
        cp.wait()


def scatter_sums(pc, acc, r3, ssem, rsem):
    copies = []
    for o in range(1, 8):
        m, x, c, dev = pc.other(o)
        src = rows_at((c * 2 + x) * ROWS + m * OWN, OWN)
        cp = rcopy(acc.at[src, :], r3.at[pc.me], ssem.at[o], rsem.at[o], dev)
        cp.start()
        copies.append(cp)
    r3[pc.me] = acc[rows_at(pc.block * ROWS + pc.m * OWN, OWN), :]
    for cp in copies:
        cp.wait()


def norm_parts(parts, gains):
    total = sum(jnp.sum(p * p, axis=-1, keepdims=True) for p in parts)
    inv = lax.rsqrt(total / (4 * WID) + NORM_EPS)
    return [p * inv * (1.0 + gains[i]) for i, p in enumerate(parts)]


def gain_rows(gains, layer, k):
    g = gains[layer, k].astype(F32)
    return [g[i:i + 1] for i in range(4)]


def after_sum(res, r3, gain):
    sums = [r3[i] + r3[4 + i] for i in range(4)]
    normed = norm_parts(sums, gain)
    return [(res[i].astype(F32) + normed[i]).astype(BF16) for i in range(4)]


def next_norm(mids, gain):
    return [p.astype(BF16) for p in norm_parts([p.astype(F32) for p in mids], gain)]


def loop(n, body):
    lax.fori_loop(0, n, lambda t, z: (body(t), z)[1], 0)


def project(pc, s, hall, w_hbm_at, out):
    keep, away = pc.c * 64, (1 - pc.c) * 64
    d2d = lambda t: rcopy(s["qp"].at[t, rows_at(away, 64), :], s["qr1"].at[t], s["q_s"].at[0, t], s["q_r"].at[0, t], pc.partner)
    xco = lambda t: rcopy(s["qs1"].at[t], s["qr2"].at[t], s["q_s"].at[1, t], s["q_r"].at[1, t], pc.xpeer)

    def second(k):
        d2d(k).wait_recv()
        o = 1 - pc.x
        s["qs1"][k] = s["qp"][k, rows_at(keep + o * ROWS, ROWS), :] + s["qr1"][k, rows_at(o * ROWS, ROWS), :]
        xco(k).start()

    for t in range(NQ):
        pltpu.make_async_copy(w_hbm_at(t), s["wq"].at[t], s["wq_sem"].at[t]).wait()
        s["qp"][t] = jnp.dot(hall[...], s["wq"][t], preferred_element_type=F32)
        d2d(t).start()
        if t:
            second(t - 1)
    second(NQ - 1)
    for t in range(NQ):
        xco(t).wait_recv()
        own = s["qp"][t, rows_at(keep + pc.x * ROWS, ROWS), :] + s["qr1"][t, rows_at(pc.x * ROWS, ROWS), :]
        out[:, t * QCH:(t + 1) * QCH] = own + s["qr2"][t]
    for t in range(NQ):
        d2d(t).wait_send()
        xco(t).wait_send()


def start_project_weights(s, w_hbm_at):
    for t in range(NQ):
        pltpu.make_async_copy(w_hbm_at(t), s["wq"].at[t], s["wq_sem"].at[t]).start()


def feed_forward(pc, s, layer, hall, wg, wu, wd, acc):
    keep, away = pc.c * 64, (1 - pc.c) * 64

    def cols(t):
        return pl.ds(pl.multiple_of(t * CH, CH), CH)

    def w_copy(i, t):
        ref = (wg, wu)[i]
        return pltpu.make_async_copy(ref.at[layer, :, cols(t)], s["w"].at[t % WSLOTS, i], s["w_sem"].at[t % WSLOTS, i])

    def wd_copy(t):
        return pltpu.make_async_copy(wd.at[layer, :, cols(t)], s["wd"].at[t], s["wd_sem"].at[t])

    def sems(i, t):
        return s["f_s"].at[i, t], s["f_r"].at[i, t]

    d2d = lambda t: rcopy(s["p"].at[t, :, rows_at(away, 64), :], s["r1"].at[t], *sems(0, t), pc.partner)
    xco = lambda t: rcopy(s["s1"].at[t], s["r2"].at[t], *sems(1, t), pc.xpeer)
    mine, cross = rows_at(pc.block * ROWS, ROWS), rows_at(pc.xblock * ROWS, ROWS)
    ux = lambda t: rcopy(s["u"].at[t, mine, :], s["u"].at[t, mine, :], *sems(2, t), pc.xpeer)
    up = lambda t: rcopy(s["u"].at[t, mine, :], s["u"].at[t, mine, :], *sems(3, t), pc.partner)
    uf = lambda t: rcopy(s["u"].at[t, cross, :], s["u"].at[t, cross, :], *sems(4, t), pc.partner)

    def step(t):
        @pl.when(t < NC)
        def _():
            for i in range(2):
                w_copy(i, t).wait()
                s["p"][t, i] = jnp.dot(hall[...], s["w"][t % WSLOTS, i], preferred_element_type=F32)
            d2d(t).start()

            @pl.when(t + WSLOTS < NC)
            def _():
                for i in range(2):
                    w_copy(i, t + WSLOTS).start()

            wd_copy(t).start()

        @pl.when((t >= 1) & (t < NC + 1))
        def _():
            k = t - 1
            d2d(k).wait_recv()
            o = 1 - pc.x
            for i in range(2):
                s["s1"][k, i] = s["p"][k, i, rows_at(keep + o * ROWS, ROWS), :] + s["r1"][k, i, rows_at(o * ROWS, ROWS), :]
            xco(k).start()

        @pl.when((t >= 3) & (t < NC + 3))
        def _():
            k = t - 3
            xco(k).wait_recv()
            g, u = [
                s["p"][k, i, rows_at(keep + pc.x * ROWS, ROWS), :] + s["r1"][k, i, rows_at(pc.x * ROWS, ROWS), :] + s["r2"][k, i]
                for i in range(2)
            ]
            s["u"][k, mine, :] = (jax.nn.gelu(g, approximate=True) * u).astype(BF16)
            ux(k).start()
            up(k).start()

        @pl.when((t >= 5) & (t < NC + 5))
        def _():
            k = t - 5
            rcopy(s["u"].at[k, cross, :], s["u"].at[k, cross, :], *sems(2, k), pc.xpeer).wait_recv()
            uf(k).start()

        @pl.when(t >= 6)
        def _():
            k = t - 6
            up(k).wait_recv()
            uf(k).wait_recv()
            wd_copy(k).wait()
            acc[...] += lax.dot_general(s["u"][k], s["wd"][k], NT, preferred_element_type=F32)

    acc[...] = jnp.zeros_like(acc)
    loop(NC + 6, step)

    def drain(t):
        for c in (d2d, xco, ux, up, uf):
            c(t).wait_send()

    loop(NC, drain)


def start_ff_weights(s, layer, wg, wu):
    for t in range(WSLOTS):
        for i, ref in enumerate((wg, wu)):
            pltpu.make_async_copy(ref.at[layer, :, pl.ds(t * CH, CH)], s["w"].at[t, i], s["w_sem"].at[t, i]).start()


def gather_heads(pc, s, o_ref):
    mine, cross = rows_at(pc.block * ROWS, ROWS), rows_at(pc.xblock * ROWS, ROWS)
    cs = lambda t: pl.ds(t * OCH, OCH)
    of = s["o"]
    ox, op, fw = [], [], []
    for t in range(NO):
        a = rcopy(o_ref.at[:, cs(t)], of.at[t, mine, :], s["o_s"].at[0, t], s["o_r"].at[0, t], pc.xpeer)
        b = rcopy(o_ref.at[:, cs(t)], of.at[t, mine, :], s["o_s"].at[1, t], s["o_r"].at[1, t], pc.partner)
        a.start()
        b.start()
        ox.append(a)
        op.append(b)
    for t in range(NO):
        of[t, mine, :] = o_ref[:, cs(t)]
    for t in range(NO):
        rcopy(of.at[t, cross, :], of.at[t, cross, :], s["o_s"].at[0, t], s["o_r"].at[0, t], pc.xpeer).wait_recv()
        f = rcopy(of.at[t, cross, :], of.at[t, cross, :], s["o_s"].at[2, t], s["o_r"].at[2, t], pc.partner)
        f.start()
        fw.append(f)
    return ox, op, fw


def qkv_at(w, layer):
    return lambda t: w.at[layer, :, pl.ds(t * QCH, QCH)]


def first_kernel(names, res, gains, wqkv, out, *scratch):
    s = dict(zip(names, scratch))
    pc = Place()
    at = qkv_at(wqkv, 0)
    start_project_weights(s, at)
    barrier_all(pc)
    h = next_norm([res[i] for i in range(4)], gain_rows(gains, 0, 0))
    spread_rows(pc, h, s["h2send"], s["hall2"], s["h2_s"], s["h2_r"])
    project(pc, s, s["hall2"], at, out)


def layer_kernel(names, layer, last, *refs):
    n_in = 7 if last else 8
    res, gains, o_in, wo, wg, wu, wd = refs[:7]
    wqkv = None if last else refs[7]
    res_out = refs[n_in]
    qkv_out = None if last else refs[n_in + 1]
    s = dict(zip(names, refs[n_in + (1 if last else 2):]))
    pc = Place()
    wo_copy = pltpu.make_async_copy(wo.at[layer], s["wo"], s["wo_sem"])
    wo_copy.start()
    start_ff_weights(s, layer, wg, wu)
    barrier_all(pc)
    acc = s["acc"]
    ox, op, fw = gather_heads(pc, s, o_in)
    wo_copy.wait()
    for t in range(NO):
        op[t].wait_recv()
        fw[t].wait_recv()
        total = None
        for j in range(4):
            part = lax.dot_general(s["o"][t, :, j * 256:(j + 1) * 256], s["wo"][t * 4 + j], NT, preferred_element_type=F32)
            total = part if total is None else total + part
        if t == 0:
            acc[...] = total
        else:
            acc[...] += total
    for cp in ox + op + fw:
        cp.wait_send()
    scatter_sums(pc, acc, s["r3"], s["sc_s"], s["sc_r"])
    mids = after_sum([res[i] for i in range(4)], s["r3"], gain_rows(gains, layer, 1))
    for i in range(4):
        s["mid"][i] = mids[i]
    spread_rows(pc, next_norm(mids, gain_rows(gains, layer, 2)), s["hsend"], s["hall"], s["h_s"], s["h_r"])
    if not last:
        at = qkv_at(wqkv, layer + 1)
        start_project_weights(s, at)
    feed_forward(pc, s, layer, s["hall"], wg, wu, wd, s["acc2"])
    scatter_sums(pc, s["acc2"], s["r32"], s["sc2_s"], s["sc2_r"])
    outs = after_sum([s["mid"][i] for i in range(4)], s["r32"], gain_rows(gains, layer, 3))
    if last:
        for i in range(4):
            s["fin"][i] = outs[i]
        peer = pc.other(4)[3]
        cp = rcopy(s["fin"], res_out.at[pc.m], s["fin_s"], s["fin_r"], peer)
        cp.start()
        for i in range(4):
            res_out[pc.m, i] = outs[i]
        cp.wait()
    else:
        for i in range(4):
            res_out[i] = outs[i]
        h = next_norm(outs, gain_rows(gains, layer + 1, 0))
        spread_rows(pc, h, s["h2send"], s["hall2"], s["h2_s"], s["h2_r"])
        project(pc, s, s["hall2"], at, qkv_out)


def q_scratch():
    dma = pltpu.SemaphoreType.DMA
    return {
        "wq": pltpu.VMEM((NQ, WID, QCH), BF16), "wq_sem": dma((NQ,)),
        "qp": pltpu.VMEM((NQ, ALL, QCH), F32), "qr1": pltpu.VMEM((NQ, 64, QCH), F32),
        "qs1": pltpu.VMEM((NQ, ROWS, QCH), F32), "qr2": pltpu.VMEM((NQ, ROWS, QCH), F32),
        "q_s": dma((2, NQ)), "q_r": dma((2, NQ)),
        "h2send": pltpu.VMEM((4, OWN, WID), BF16), "hall2": pltpu.VMEM((ALL, WID), BF16),
        "h2_s": dma((8,)), "h2_r": dma((8,)),
    }


def layer_scratch(last):
    dma = pltpu.SemaphoreType.DMA
    out = {
        "wo": pltpu.VMEM((8, WID, 256), BF16), "wo_sem": dma(()),
        "o": pltpu.VMEM((NO, ALL, OCH), BF16), "o_s": dma((3, NO)), "o_r": dma((3, NO)),
        "acc": pltpu.VMEM((ALL, WID), F32), "acc2": pltpu.VMEM((ALL, WID), F32),
        "r3": pltpu.VMEM((8, OWN, WID), F32), "r32": pltpu.VMEM((8, OWN, WID), F32),
        "sc_s": dma((8,)), "sc_r": dma((8,)), "sc2_s": dma((8,)), "sc2_r": dma((8,)),
        "mid": pltpu.VMEM((4, OWN, WID), BF16),
        "hsend": pltpu.VMEM((4, OWN, WID), BF16), "hall": pltpu.VMEM((ALL, WID), BF16),
        "h_s": dma((8,)), "h_r": dma((8,)),
        "w": pltpu.VMEM((WSLOTS, 2, WID, CH), BF16), "w_sem": dma((WSLOTS, 2)),
        "wd": pltpu.VMEM((NC, WID, CH), BF16), "wd_sem": dma((NC,)),
        "p": pltpu.VMEM((NC, 2, ALL, CH), F32), "r1": pltpu.VMEM((NC, 2, 64, CH), F32),
        "s1": pltpu.VMEM((NC, 2, ROWS, CH), F32), "r2": pltpu.VMEM((NC, 2, ROWS, CH), F32),
        "u": pltpu.VMEM((NC, ALL, CH), BF16),
        "f_s": dma((5, NC)), "f_r": dma((5, NC)),
    }
    if last:
        out.update({"fin": pltpu.VMEM((4, OWN, WID), BF16), "fin_s": dma(()), "fin_r": dma(())})
    else:
        out.update(q_scratch())
    return out


VM = pl.BlockSpec(memory_space=pltpu.VMEM)
HB = pl.BlockSpec(memory_space=pl.ANY)


def params(cid):
    return pltpu.CompilerParams(collective_id=cid, has_side_effects=True, vmem_limit_bytes=67043328)


def call_first(res, gains, wqkv):
    sc = q_scratch()
    return pl.pallas_call(
        functools.partial(first_kernel, tuple(sc)),
        out_shape=jax.ShapeDtypeStruct((ROWS, QW), F32),
        in_specs=[VM, VM, HB], out_specs=VM, scratch_shapes=list(sc.values()),
        compiler_params=params(0), name="qkv0",
    )(res, gains, wqkv)


def call_layer(layer, last, res, gains, o, wo, wg, wu, wd, wqkv):
    sc = layer_scratch(last)
    ins = [res, gains, o, wo, wg, wu, wd] + ([] if last else [wqkv])
    block = jax.ShapeDtypeStruct((2, 4, OWN, WID) if last else (4, OWN, WID), BF16)
    outs = [block] if last else [block, jax.ShapeDtypeStruct((ROWS, QW), F32)]
    return pl.pallas_call(
        functools.partial(layer_kernel, tuple(sc), layer, last),
        out_shape=outs,
        in_specs=[VM, VM, VM] + [HB] * (len(ins) - 3), out_specs=[VM] * len(outs), scratch_shapes=list(sc.values()),
        compiler_params=params(1 + layer), name=f"layer{layer}",
    )(*ins)


def rotary(hidden, cos_t, sin_t):
    half_dim = hidden.shape[-1] // 2
    first_half = hidden[..., :half_dim]
    second_half = hidden[..., half_dim:]
    return jnp.concatenate([first_half * cos_t - second_half * sin_t, second_half * cos_t + first_half * sin_t], axis=-1)


def rope_tables(positions, head_dim):
    inv_freq = ROPE_BASE ** (-jnp.arange(0, head_dim, 2).astype(jnp.float32) / head_dim)
    angles = positions.astype(jnp.float32)[:, None] * inv_freq[None, :]
    return jnp.cos(angles)[:, None, :], jnp.sin(angles)[:, None, :]


def attend(qkv, positions, tables, k_cache, v_cache, is_local):
    n_rows, cache_len, kv_loc, head_dim = k_cache.shape
    cos_t, sin_t = tables
    q_proj = qkv[:, :2048].reshape(n_rows, 8, head_dim)
    k_proj = qkv[:, 2048:3072].reshape(n_rows, 4, head_dim)
    v_new = qkv[:, 3072:].reshape(n_rows, 4, head_dim).astype(BF16)
    q_new = (rotary(q_proj, cos_t, sin_t) * head_dim ** -0.5).astype(BF16)
    k_new = rotary(k_proj, cos_t, sin_t).astype(BF16)
    group_size = q_new.shape[1] // kv_loc
    slot_ids = jnp.arange(cache_len)
    if is_local:
        slot_now = positions % cache_len
        valid_mask = ((positions[:, None] - slot_ids[None, :]) % cache_len) <= positions[:, None]
    else:
        slot_now = positions
        valid_mask = slot_ids[None, :] <= positions[:, None]
    slot_hit = (slot_ids[None, :] == slot_now[:, None])[:, :, None, None]
    k_cache = jnp.where(slot_hit, k_new[:, None], k_cache)
    v_cache = jnp.where(slot_hit, v_new[:, None], v_cache)
    q_grp = q_new.reshape(n_rows, kv_loc, group_size, head_dim)
    scores = jnp.einsum("bkgd,btkd->bkgt", q_grp, k_cache, preferred_element_type=jnp.float32)
    scores = SOFT_CAP * jnp.tanh(scores / SOFT_CAP)
    scores = jnp.where(valid_mask[:, None, None, :], scores, -1e30)
    attn_prob = jax.nn.softmax(scores, axis=-1).astype(jnp.bfloat16)
    head_out = jnp.einsum("bkgt,btkd->bkgd", attn_prob, v_cache, preferred_element_type=jnp.float32)
    return head_out.astype(jnp.bfloat16).reshape(n_rows, 2048), k_cache, v_cache


def solution(mesh):
    def device_step(hidden, positions, k_local, v_local, k_global, v_global, w_q, w_k, w_v, w_o, w_gate, w_up, w_down, norm_gains):
        m = lax.axis_index("model")
        own = lax.dynamic_slice_in_dim(hidden[:, 0, :], m * OWN, OWN, 0)
        res = own.reshape(OWN, 4, WID).transpose(1, 0, 2)
        gains = norm_gains.reshape(2, 4, 4, WID)
        wqkv = jnp.concatenate([w_q.reshape(2, WID, 2048), w_k.reshape(2, WID, 1024), w_v.reshape(2, WID, 1024)], axis=2)
        wo = w_o.transpose(0, 1, 3, 2)
        wd = w_down.transpose(0, 2, 1)
        tables = rope_tables(positions, 256)
        qkv = call_first(res, gains, wqkv)
        heads, k_local, v_local = attend(qkv, positions, tables, k_local, v_local, True)
        res, qkv = call_layer(0, False, res, gains, heads, wo, w_gate, w_up, wd, wqkv)
        heads, k_global, v_global = attend(qkv, positions, tables, k_global, v_global, False)
        out = call_layer(1, True, res, gains, heads, wo, w_gate, w_up, wd, wqkv)
        out = out[0] if isinstance(out, (tuple, list)) else out
        final = out.transpose(0, 2, 1, 3).reshape(ROWS, 1, 4 * WID)
        return final, k_local, v_local, k_global, v_global

    in_specs = (ROW_SPEC, POS_SPEC, CACHE_SPEC, CACHE_SPEC, CACHE_SPEC, CACHE_SPEC, PROJ_IN_SPEC, PROJ_IN_SPEC, PROJ_IN_SPEC, PROJ_OUT_SPEC, FF_IN_SPEC, FF_IN_SPEC, FF_OUT_SPEC, GAIN_SPEC)
    out_specs = (ROW_SPEC, CACHE_SPEC, CACHE_SPEC, CACHE_SPEC, CACHE_SPEC)
    return jax.shard_map(device_step, mesh=mesh, in_specs=in_specs, out_specs=out_specs, check_vma=False)
```
